32 devices in a mesh: rep: 2 (over x), shard: 16 (over z, y, core).
Axes of the slice: x: 2, y: 2, z: 4, core: 2. Of those that a mesh axis runs over, the one named last changes fastest.
Arguments:
- tokens_x: bfloat16 [8192, 4096], P(('rep', 'shard')), may hold values from -6 to 6
- key_grad: bfloat16 [8192, 1024], P(('rep', 'shard')), may hold values from -0.06591797 to 0.06591797
- left_root: bfloat16 [64, 512, 512], P('shard'), may hold values from -1 to 3
- slot_grads: bfloat16 [64, 512, 512], P('shard'), may hold values from -6 to 6
- right_root: bfloat16 [64, 512, 512], P('shard'), may hold values from -1 to 3
- block_slot: int32 [32], replicated, may hold values from 0 to 63, as said below
Outputs:
- grad_key: float32 [4096, 1024], P('shard')
- update: bfloat16 [512, 32, 512], P('shard')
The draws below stay inside these ranges and needn't reach their ends.
Inputs may be any that keep to these rules, and one draw needn't show every extreme that they name: `block_slot`: the entries are distinct; slot v is slot v % 4 of shard index v // 4; no shard index holds more than 4 blocks, and some shard index holds exactly 4.
All inputs are finite; a program needn't handle non-finite values.
Results may differ from the reference program's by a relative error of at most 0.006.
Values may be sent and summed in bfloat16 or wider, within the bound.
A program may use at most 128 MiB of HBM per device.

```python
import jax
import jax.numpy as jnp
from jax import lax

D = 4096
KEY_WIDTH = 1024
TOK_DEV = 256
BLOCK = 512
SLOTS = 4
NBLK = 32
SLOT_ALL = 64
TOKENS = 8192


def root_matrix(key):
    first_key, second_key = jax.random.split(key)
    diagonal = jnp.exp(jax.random.uniform(first_key, (SLOT_ALL, BLOCK), jnp.float32, jnp.log(0.5), jnp.log(2.0)))
    noise = jax.random.normal(second_key, (SLOT_ALL, BLOCK, BLOCK), jnp.float32)
    symmetric = (noise + jnp.swapaxes(noise, 1, 2)) * (0.5 / (2.0 * BLOCK) ** 0.5)
    symmetric = jnp.clip(symmetric, -0.9, 0.9)
    identity = jnp.eye(BLOCK, dtype=jnp.float32)
    return (symmetric + diagonal[:, :, None] * identity[None, :, :]).astype(jnp.bfloat16)


def draw_left_root(key, part):
    return root_matrix(jax.random.fold_in(key, 11))


def draw_right_root(key, part):
    return root_matrix(jax.random.fold_in(key, 23))


def draw_block_slot(key, part):
    base_key = jax.random.fold_in(key, 37)
    first_key, second_key, third_key = jax.random.split(base_key, 3)
    full_owner = jax.random.randint(first_key, (), 0, SLOT_ALL // SLOTS)
    slot_ids = jnp.arange(SLOT_ALL, dtype=jnp.int32)
    ranking = jax.random.permutation(second_key, SLOT_ALL).astype(jnp.int32)
    ranking = jnp.where(slot_ids // SLOTS == full_owner, slot_ids % SLOTS - SLOTS, ranking)
    chosen = jnp.argsort(ranking, stable=True)[:NBLK].astype(jnp.int32)
    shuffled = jax.random.permutation(third_key, NBLK).astype(jnp.int32)
    return chosen[shuffled].astype(jnp.int32)


def strengthened(array, rng, source, target, parts, factor):
    def block_of(position):
        return (jnp.arange(array.shape[position]) // (array.shape[position] // parts)).reshape((-1,) + (1,) * (array.ndim - 1 - position))

    near = jax.random.permutation(rng, parts)[block_of(target)]
    second = (block_of(target) + parts // 2) % parts
    return jnp.where((block_of(source) == near) | (block_of(source) == second), factor * array, array)


def block_levels(own_key, shape, cuts, least, top_value):
    gain, own = 1.0, jax.random.fold_in(own_key, 6)
    for axis_at, shards_of in cuts:
        draws = jnp.exp(jax.random.uniform(jax.random.fold_in(own, axis_at), (shards_of,), jnp.float32, least / len(cuts), top_value / len(cuts)))
        gain = gain * jnp.repeat(draws, shape[axis_at] // shards_of).reshape([-1 if axis == axis_at else 1 for axis in range(len(shape))])
    return gain


def normal_values(rng, dims, scale, reach, cuts=(), kind=jnp.bfloat16):
    entries = jax.random.normal(rng, dims, jnp.float32) * scale
    if len(cuts) > 0:
        entries = block_levels(rng, dims, cuts, -0.22, 0.18) * entries
    return jnp.clip(entries, min=-reach, max=reach).astype(kind)


def noise_with(stream_key, extent, spread, reach, cuts, heavy, kind=jnp.bfloat16):
    drawn = spread * jax.random.normal(stream_key, extent, jnp.float32)
    if cuts:
        drawn = drawn * block_levels(stream_key, extent, cuts, -0.22, 0.18)
    return jnp.clip(strengthened(drawn, jax.random.fold_in(stream_key, 3), *heavy), -reach, reach).astype(kind)


def setup_inputs(seed: int = 0) -> dict:
    keys = jax.random.split(jax.random.key(seed), 7)
    return {
        "tokens_x": noise_with(keys[0], (TOKENS, D), 1.0, 6.0, ((0, 32),), (0, 1, 32, 2.75)),
        "key_grad": normal_values(keys[1], (TOKENS, KEY_WIDTH), (TOKENS ** -0.5), 0.06591797, ((0, 32),)),
        "left_root": draw_left_root(jax.random.fold_in(keys[6], 71), 0),
        "slot_grads": normal_values(keys[3], (SLOT_ALL, BLOCK, BLOCK), 1.0, 6.0, ((0, 16),)),
        "right_root": draw_right_root(jax.random.fold_in(keys[6], 71), 0),
        "block_slot": draw_block_slot(jax.random.fold_in(keys[6], 71), 0),
    }


def reference(tokens_x, key_grad, left_root, slot_grads, right_root, block_slot):
    step_count = TOKENS // TOK_DEV
    token_blocks = tokens_x.reshape(step_count, TOK_DEV, D)
    grad_blocks = key_grad.reshape(step_count, TOK_DEV, KEY_WIDTH)

    def accumulate(total, pieces):
        rows_in, grads_in = pieces
        added = jnp.dot(rows_in.astype(jnp.float32).T, grads_in.astype(jnp.float32), preferred_element_type=jnp.float32)
        return total + added, None

    grad_key, ignored = lax.scan(accumulate, jnp.zeros((D, KEY_WIDTH), jnp.float32), (token_blocks, grad_blocks))

    def precondition(slot_index):
        left_part = jnp.dot(left_root[slot_index].astype(jnp.float32), slot_grads[slot_index].astype(jnp.float32), preferred_element_type=jnp.float32).astype(jnp.bfloat16)
        return jnp.dot(left_part.astype(jnp.float32), right_root[slot_index].astype(jnp.float32), preferred_element_type=jnp.float32).astype(jnp.bfloat16)

    blocks = lax.map(precondition, block_slot)
    update = jnp.transpose(blocks, (1, 0, 2))
    return grad_key, update
```

```python
import functools

import jax
import jax.numpy as jnp
from jax import lax
from jax.experimental import pallas as pl
from jax.experimental.pallas import tpu as pltpu
from jax.sharding import PartitionSpec as P

MESH = pl.DeviceIdType.MESH
GROUP = 4
PIECES = 4


def column_term(features, cotangent):
    return lax.dot_general(
        features, cotangent, (((0,), (0,)), ((), ())), preferred_element_type=jnp.float32
    )


def precondition(left_block, grad_block, right_block):
    left_part = jnp.einsum(
        "sij,sjk->sik", left_block, grad_block, preferred_element_type=jnp.float32
    ).astype(jnp.bfloat16)
    return jnp.einsum(
        "sij,sjk->isk", left_part, right_block, preferred_element_type=jnp.float32
    ).astype(jnp.bfloat16)


def plain_shards(tokens_x, key_grad, left_root, slot_grads, right_root, block_slot):
    n_shard = lax.axis_size("shard")
    n_rep = lax.axis_size("rep")
    own_rows = lax.psum_scatter(
        column_term(tokens_x, key_grad), "shard", scatter_dimension=0, tiled=True
    )
    grad_key = lax.psum(own_rows, "rep")
    slot_count = left_root.shape[0]
    half_slots = slot_count // n_rep
    first_slot = lax.axis_index("rep") * half_slots

    def own_half(values):
        return lax.dynamic_slice_in_dim(values, first_slot, half_slots, 0)

    product = precondition(own_half(left_root), own_half(slot_grads), own_half(right_root))
    received = lax.all_to_all(product, "shard", split_axis=0, concat_axis=1, tiled=True)
    joined = lax.all_gather(received, "rep", axis=1, tiled=True)
    owner = block_slot // slot_count
    within = block_slot % slot_count
    position = (
        within // half_slots * (n_shard * half_slots) + owner * half_slots + within % half_slots
    )
    update = jnp.take(joined, position, axis=1)
    return (grad_key, update)


def remote(src, dst, send_sem, recv_sem, axis, index):
    return pltpu.make_async_remote_copy(
        src_ref=src,
        dst_ref=dst,
        send_sem=send_sem,
        recv_sem=recv_sem,
        device_id={axis: index},
        device_id_type=MESH,
    )


def far_first(outer):
    return sorted(range(1, outer), key=lambda off: -min(off, outer - off)) + [0]


def kernel(
    n, slot_ref, x_ref, g_ref, lr_ref, sg_ref, rr_ref, og_ref, ou_ref,
    x_all, g_all, lr, sg, rr, prod, upd, mine, theirs, part, landed, own, half_out, half_in,
    local_sem, x_local, barrier_free, g_send, g_recv, x_send, x_recv, u_send, u_recv,
    z_send, z_recv, r_send, r_recv, v_send, v_recv,
):
    me = lax.axis_index("shard")
    rep = lax.axis_index("rep")
    other_rep = 1 - rep
    q = me % GROUP
    z = me // GROUP
    base = z * GROUP
    outer = n // GROUP
    q_core = q + 1 - 2 * (q % 2)
    q_far = (q + 2) % GROUP
    q_both = (q_core + 2) % GROUP
    tok = x_ref.shape[0]
    cols = x_ref.shape[1] // n
    slots = lr_ref.shape[0]
    blocks = slot_ref.shape[0]
    offsets = far_first(outer)

    def tokens_of(index):
        return pl.ds(index * tok, tok)

    def columns(d, index):
        return pl.ds(pl.multiple_of((d * GROUP + index) * cols, 128), cols)

    copy_lr = pltpu.make_async_copy(lr_ref.at[:, :, rep], lr, local_sem.at[0])
    copy_sg = pltpu.make_async_copy(sg_ref, sg, local_sem.at[1])
    copy_rr = pltpu.make_async_copy(rr_ref, rr, local_sem.at[2])
    copy_g = pltpu.make_async_copy(g_ref, g_all.at[tokens_of(q)], local_sem.at[3])
    copies_x = []
    for d in range(outer):
        copies_x.append(
            pltpu.make_async_copy(
                x_ref.at[:, columns(d, q)], x_all.at[d, tokens_of(q)], x_local.at[d]
            )
        )
    copy_lr.start()
    copy_sg.start()
    copy_rr.start()
    copy_g.start()
    for copy in copies_x:
        copy.start()

    barrier = pltpu.get_barrier_semaphore()
    for step in range(1, n):
        pl.semaphore_signal(
            barrier, inc=1, device_id={"shard": (me + step) % n}, device_id_type=MESH
        )
    pl.semaphore_signal(barrier, inc=1, device_id={"rep": other_rep}, device_id_type=MESH)
    pl.semaphore_wait(barrier, n)

    sent = []

    def send(*args):
        copy = remote(*args)
        copy.start()
        sent.append(copy)

    for order, target in enumerate((q_far, q_core)):
        send(
            g_ref, g_all.at[tokens_of(q)], g_send.at[order], g_recv.at[q], "shard", base + target
        )
    for order, off in enumerate(offsets):
        d = (z + off) % outer
        for place, target in enumerate((q_far, q_both, q_core)):
            send(
                x_ref.at[:, columns(d, target)],
                x_all.at[d, tokens_of(q)],
                x_send.at[order, place],
                x_recv.at[q, d],
                "shard",
                base + target,
            )

    copy_lr.wait()
    copy_sg.wait()
    copy_rr.wait()
    height = lr.shape[2]
    width = lr.shape[3]
    for s in range(slots):
        left = jnp.dot(
            lr[s].reshape(n * height, width), sg[s], preferred_element_type=jnp.float32
        ).astype(jnp.bfloat16)
        both = jnp.dot(left, rr[s], preferred_element_type=jnp.float32).astype(jnp.bfloat16)
        prod[:, s] = both.reshape(n, height, width)
    for step in range(1, n):
        target = (me + step) % n
        send(
            prod.at[target],
            upd.at[pl.ds(me * slots, slots)],
            u_send.at[step],
            u_recv.at[me],
            "shard",
            target,
        )
    upd[pl.ds(me * slots, slots)] = prod[me]

    def arrive(dst, recv_sem):
        remote(dst, dst, barrier_free, recv_sem, "shard", (me + 1) % n).wait_recv()

    arrive(g_all.at[tokens_of(q_far)], g_recv.at[q_far])
    send(
        g_all.at[tokens_of(q_far)],
        g_all.at[tokens_of(q_far)],
        g_send.at[2],
        g_recv.at[q_far],
        "shard",
        base + q_core,
    )
    copy_g.wait()
    arrive(g_all.at[tokens_of(q_core)], g_recv.at[q_core])
    arrive(g_all.at[tokens_of(q_both)], g_recv.at[q_both])
    for copy in copies_x:
        copy.wait()

    piece = own.shape[2]
    for order, off in enumerate(offsets):
        d = (z + off) % outer
        for source in (q_core, q_far, q_both):
            arrive(x_all.at[d, tokens_of(source)], x_recv.at[source, d])
        for p in range(PIECES):
            value = lax.dot_general(
                x_all[d],
                g_all[:, p * piece : (p + 1) * piece],
                (((0,), (0,)), ((), ())),
                preferred_element_type=jnp.float32,
            )
            if off == 0:
                own[p] = value
            else:
                part[order, p] = value.astype(jnp.bfloat16)
                send(
                    part.at[order, p],
                    landed.at[z, p],
                    z_send.at[order, p],
                    z_recv.at[z, p],
                    "shard",
                    d * GROUP + q,
                )

    for step in range(1, n):
        source = (me + n - step) % n
        arrive(upd.at[pl.ds(source * slots, slots)], u_recv.at[source])

    def pick(b, carry):
        mine[b] = upd[slot_ref[b]]
        return carry

    lax.fori_loop(0, blocks, pick, 0)
    send(mine, theirs, v_send, v_recv, "rep", other_rep)
    ou_ref[rep] = mine[...]

    for p in range(PIECES):
        total = own[p]
        for off in offsets[:-1]:
            source = (z + outer - off) % outer
            arrive(landed.at[source, p], z_recv.at[source, p])
            total = total + landed[source, p].astype(jnp.float32)
        half_out[p] = total.astype(jnp.bfloat16)
        send(half_out.at[p], half_in.at[p], r_send.at[p], r_recv.at[p], "rep", other_rep)

    arrive(theirs, v_recv)
    ou_ref[other_rep] = theirs[...]
    for p in range(PIECES):
        arrive(half_in.at[p], r_recv.at[p])
        og_ref[:, p * piece : (p + 1) * piece] = half_out[p].astype(jnp.float32) + half_in[
            p
        ].astype(jnp.float32)
    for copy in sent:
        copy.wait_send()


def fused_shards(tokens_x, key_grad, left_root, slot_grads, right_root, block_slot):
    n = lax.axis_size("shard")
    n_rep = lax.axis_size("rep")
    outer = n // GROUP
    tok, d_model = tokens_x.shape
    key_width = key_grad.shape[1]
    cols = d_model // n
    slots, order_b, width = left_root.shape
    height = order_b // n // n_rep
    blocks = block_slot.shape[0]
    piece = key_width // PIECES
    bf16, f32 = jnp.bfloat16, jnp.float32
    dma = pltpu.SemaphoreType.DMA
    any_spec = pl.BlockSpec(memory_space=pl.ANY)
    vmem_spec = pl.BlockSpec(memory_space=pltpu.VMEM)
    grad_key, rows = pl.pallas_call(
        functools.partial(kernel, n),
        out_shape=(
            jax.ShapeDtypeStruct((cols, key_width), f32),
            jax.ShapeDtypeStruct((n_rep, blocks, height, width), bf16),
        ),
        in_specs=[pl.BlockSpec(memory_space=pltpu.SMEM)] + [any_spec] * 5,
        out_specs=(vmem_spec, vmem_spec),
        scratch_shapes=[
            pltpu.VMEM((outer, GROUP * tok, cols), bf16),
            pltpu.VMEM((GROUP * tok, key_width), bf16),
            pltpu.VMEM((slots, n, height, width), bf16),
            pltpu.VMEM(slot_grads.shape, bf16),
            pltpu.VMEM(right_root.shape, bf16),
            pltpu.VMEM((n, slots, height, width), bf16),
            pltpu.VMEM((n * slots, height, width), bf16),
            pltpu.VMEM((blocks, height, width), bf16),
            pltpu.VMEM((blocks, height, width), bf16),
            pltpu.VMEM((outer - 1, PIECES, cols, piece), bf16),
            pltpu.VMEM((outer, PIECES, cols, piece), bf16),
            pltpu.VMEM((PIECES, cols, piece), f32),
            pltpu.VMEM((PIECES, cols, piece), bf16),
            pltpu.VMEM((PIECES, cols, piece), bf16),
            dma((4,)),
            dma((outer,)),
            dma,
            dma((3,)),
            dma((GROUP,)),
            dma((outer, 3)),
            dma((GROUP, outer)),
            dma((n,)),
            dma((n,)),
            dma((outer - 1, PIECES)),
            dma((outer, PIECES)),
            dma((PIECES,)),
            dma((PIECES,)),
            dma,
            dma,
        ],
        compiler_params=pltpu.CompilerParams(
            collective_id=0, has_side_effects=True, vmem_limit_bytes=60 * 1024 * 1024
        ),
    )(
        block_slot,
        tokens_x,
        key_grad,
        left_root.reshape(slots, n, n_rep, height, width),
        slot_grads,
        right_root,
    )
    update = jnp.transpose(rows, (0, 2, 1, 3)).reshape(n_rep * height, blocks, width)
    return (grad_key, update)


def shards(tokens_x, key_grad, left_root, slot_grads, right_root, block_slot):
    n = lax.axis_size("shard")
    n_rep = lax.axis_size("rep")
    aligned = (
        n_rep == 2
        and n % GROUP == 0
        and n > GROUP
        and tokens_x.shape[1] % (n * 128) == 0
        and key_grad.shape[1] % (PIECES * 128) == 0
        and tokens_x.shape[0] % 16 == 0
        and left_root.shape[1] % (n * n_rep * 16) == 0
        and left_root.shape[2] % 128 == 0
    )
    program = fused_shards if aligned else plain_shards
    return program(tokens_x, key_grad, left_root, slot_grads, right_root, block_slot)


def solution(mesh):
    return jax.shard_map(
        shards,
        mesh=mesh,
        in_specs=(
            P(("rep", "shard"), None),
            P(("rep", "shard"), None),
            P("shard", None, None),
            P("shard", None, None),
            P("shard", None, None),
            P(),
        ),
        out_specs=(P("shard", None), P("shard", None, None)),
        check_vma=False,
    )
```

```python
import functools

import jax
import jax.numpy as jnp
from jax import lax
from jax.experimental import pallas as pl
from jax.experimental.pallas import tpu as pltpu
from jax.sharding import PartitionSpec as P

MESH = pl.DeviceIdType.MESH
GROUP = 4
PIECES = 2


def column_term(features, cotangent):
    return lax.dot_general(
        features, cotangent, (((0,), (0,)), ((), ())), preferred_element_type=jnp.float32
    )


def precondition(left_block, grad_block, right_block):
    left_part = jnp.einsum(
        "sij,sjk->sik", left_block, grad_block, preferred_element_type=jnp.float32
    ).astype(jnp.bfloat16)
    return jnp.einsum(
        "sij,sjk->isk", left_part, right_block, preferred_element_type=jnp.float32
    ).astype(jnp.bfloat16)


def plain_shards(tokens_x, key_grad, left_root, slot_grads, right_root, block_slot):
    n_shard = lax.axis_size("shard")
    n_rep = lax.axis_size("rep")
    own_rows = lax.psum_scatter(
        column_term(tokens_x, key_grad), "shard", scatter_dimension=0, tiled=True
    )
    grad_key = lax.psum(own_rows, "rep")
    slot_count = left_root.shape[0]
    half_slots = slot_count // n_rep
    first_slot = lax.axis_index("rep") * half_slots

    def own_half(values):
        return lax.dynamic_slice_in_dim(values, first_slot, half_slots, 0)

    product = precondition(own_half(left_root), own_half(slot_grads), own_half(right_root))
    received = lax.all_to_all(product, "shard", split_axis=0, concat_axis=1, tiled=True)
    joined = lax.all_gather(received, "rep", axis=1, tiled=True)
    owner = block_slot // slot_count
    within = block_slot % slot_count
    position = (
        within // half_slots * (n_shard * half_slots) + owner * half_slots + within % half_slots
    )
    update = jnp.take(joined, position, axis=1)
    return (grad_key, update)


def remote(src, dst, send_sem, recv_sem, axis, index):
    return pltpu.make_async_remote_copy(
        src_ref=src,
        dst_ref=dst,
        send_sem=send_sem,
        recv_sem=recv_sem,
        device_id={axis: index},
        device_id_type=MESH,
    )


def far_first(outer):
    return sorted(range(1, outer), key=lambda off: -min(off, outer - off)) + [0]


def kernel(
    n, slot_ref, x_ref, g_ref, lr_ref, sg_ref, rr_ref, og_ref, ou_ref,
    x_all, g_all, lr, sg, rr, prod, upd, mine, theirs, part, met, kept, passed, landed, half_out, half_in,
    local_sem, x_local, barrier_free, g_send, g_recv, x_send, x_recv, u_send, u_recv,
    a_send, a_recv, z_send, z_recv, r_send, r_recv, v_send, v_recv,
):
    me = lax.axis_index("shard")
    rep = lax.axis_index("rep")
    other_rep = 1 - rep
    q = me % GROUP
    z = me // GROUP
    base = z * GROUP
    outer = n // GROUP
    q_core = q + 1 - 2 * (q % 2)
    q_far = (q + 2) % GROUP
    q_both = (q_core + 2) % GROUP
    tok = x_ref.shape[0]
    cols = x_ref.shape[1] // n
    slots = lr_ref.shape[0]
    blocks = slot_ref.shape[0]
    offsets = far_first(outer)

    def tokens_of(index):
        return pl.ds(index * tok, tok)

    def columns(d, index):
        return pl.ds(pl.multiple_of((d * GROUP + index) * cols, 128), cols)

    copy_lr = pltpu.make_async_copy(lr_ref.at[:, :, rep], lr, local_sem.at[0])
    copy_sg = pltpu.make_async_copy(sg_ref, sg, local_sem.at[1])
    copy_rr = pltpu.make_async_copy(rr_ref, rr, local_sem.at[2])
    copy_g = pltpu.make_async_copy(g_ref, g_all.at[tokens_of(q)], local_sem.at[3])
    copies_x = []
    for d in range(outer):
        copies_x.append(
            pltpu.make_async_copy(
                x_ref.at[:, columns(d, q)], x_all.at[d, tokens_of(q)], x_local.at[d]
            )
        )
    copy_lr.start()
    copy_sg.start()
    copy_rr.start()
    copy_g.start()
    for copy in copies_x:
        copy.start()

    barrier = pltpu.get_barrier_semaphore()
    for step in range(1, n):
        pl.semaphore_signal(
            barrier, inc=1, device_id={"shard": (me + step) % n}, device_id_type=MESH
        )
    pl.semaphore_signal(barrier, inc=1, device_id={"rep": other_rep}, device_id_type=MESH)
    pl.semaphore_wait(barrier, n)

    sent = []

    def send(*args):
        copy = remote(*args)
        copy.start()
        sent.append(copy)

    for order, target in enumerate((q_far, q_core)):
        send(
            g_ref, g_all.at[tokens_of(q)], g_send.at[order], g_recv.at[q], "shard", base + target
        )
    for order, off in enumerate(offsets):
        d = (z + off) % outer
        for place, target in enumerate((q_far, q_both, q_core)):
            send(
                x_ref.at[:, columns(d, target)],
                x_all.at[d, tokens_of(q)],
                x_send.at[order, place],
                x_recv.at[q, d],
                "shard",
                base + target,
            )

    copy_lr.wait()
    copy_sg.wait()
    copy_rr.wait()
    height = lr.shape[2]
    width = lr.shape[3]
    for s in range(slots):
        left = jnp.dot(
            lr[s].reshape(n * height, width), sg[s], preferred_element_type=jnp.float32
        ).astype(jnp.bfloat16)
        both = jnp.dot(left, rr[s], preferred_element_type=jnp.float32).astype(jnp.bfloat16)
        prod[:, s] = both.reshape(n, height, width)
    for step in range(1, n):
        target = (me + step) % n
        send(
            prod.at[target],
            upd.at[pl.ds(me * slots, slots)],
            u_send.at[step],
            u_recv.at[me],
            "shard",
            target,
        )
    upd[pl.ds(me * slots, slots)] = prod[me]

    def arrive(dst, recv_sem):
        remote(dst, dst, barrier_free, recv_sem, "shard", (me + 1) % n).wait_recv()

    arrive(g_all.at[tokens_of(q_far)], g_recv.at[q_far])
    send(
        g_all.at[tokens_of(q_far)],
        g_all.at[tokens_of(q_far)],
        g_send.at[2],
        g_recv.at[q_far],
        "shard",
        base + q_core,
    )
    copy_g.wait()
    arrive(g_all.at[tokens_of(q_core)], g_recv.at[q_core])
    arrive(g_all.at[tokens_of(q_both)], g_recv.at[q_both])
    for copy in copies_x:
        copy.wait()

    piece = kept.shape[3]
    half = PIECES * piece

    def partial(d, side):
        start = pl.multiple_of(side * half, 128)
        return lax.dot_general(
            x_all[d],
            g_all[:, pl.ds(start, half)],
            (((0,), (0,)), ((), ())),
            preferred_element_type=jnp.float32,
        )

    def place_of(side, p):
        return pl.ds(pl.multiple_of(side * half + p * piece, 128), piece)

    def pass_on(order):
        off = offsets[order]
        for p in range(PIECES):
            arrive(met.at[order, p], a_recv.at[order, p])
            total = kept[order, p] + met[order, p].astype(jnp.float32)
            if off == 0:
                kept[order, p] = total
            else:
                passed[order, p] = total.astype(jnp.bfloat16)
                send(
                    passed.at[order, p],
                    landed.at[z, p],
                    z_send.at[order, p],
                    z_recv.at[z, p],
                    "shard",
                    (z + off) % outer * GROUP + q,
                )

    for order, off in enumerate(offsets):
        d = (z + off) % outer
        for source in (q_core, q_far, q_both):
            arrive(x_all.at[d, tokens_of(source)], x_recv.at[source, d])
        value = partial(d, other_rep)
        for p in range(PIECES):
            part[order, p] = value[:, p * piece : (p + 1) * piece].astype(jnp.bfloat16)
            send(
                part.at[order, p],
                met.at[order, p],
                a_send.at[order, p],
                a_recv.at[order, p],
                "rep",
                other_rep,
            )
        value = partial(d, rep)
        for p in range(PIECES):
            kept[order, p] = value[:, p * piece : (p + 1) * piece]
        if order > 0:
            pass_on(order - 1)
    pass_on(outer - 1)

    for step in range(1, n):
        source = (me + n - step) % n
        arrive(upd.at[pl.ds(source * slots, slots)], u_recv.at[source])

    def pick(b, carry):
        mine[b] = upd[slot_ref[b]]
        return carry

    lax.fori_loop(0, blocks, pick, 0)
    send(mine, theirs, v_send, v_recv, "rep", other_rep)
    ou_ref[rep] = mine[...]

    for p in range(PIECES):
        total = kept[outer - 1, p]
        for off in offsets[:-1]:
            source = (z + outer - off) % outer
            arrive(landed.at[source, p], z_recv.at[source, p])
            total = total + landed[source, p].astype(jnp.float32)
        half_out[p] = total.astype(jnp.bfloat16)
        send(half_out.at[p], half_in.at[p], r_send.at[p], r_recv.at[p], "rep", other_rep)

    for p in range(PIECES):
        og_ref[:, place_of(rep, p)] = half_out[p]
    arrive(theirs, v_recv)
    ou_ref[other_rep] = theirs[...]
    for p in range(PIECES):
        arrive(half_in.at[p], r_recv.at[p])
        og_ref[:, place_of(other_rep, p)] = half_in[p]
    for copy in sent:
        copy.wait_send()


def fused_shards(tokens_x, key_grad, left_root, slot_grads, right_root, block_slot):
    n = lax.axis_size("shard")
    n_rep = lax.axis_size("rep")
    outer = n // GROUP
    tok, d_model = tokens_x.shape
    key_width = key_grad.shape[1]
    cols = d_model // n
    slots, order_b, width = left_root.shape
    height = order_b // n // n_rep
    blocks = block_slot.shape[0]
    piece = key_width // n_rep // PIECES
    bf16, f32 = jnp.bfloat16, jnp.float32
    dma = pltpu.SemaphoreType.DMA
    any_spec = pl.BlockSpec(memory_space=pl.ANY)
    vmem_spec = pl.BlockSpec(memory_space=pltpu.VMEM)
    sums, rows = pl.pallas_call(
        functools.partial(kernel, n),
        out_shape=(
            jax.ShapeDtypeStruct((cols, key_width), bf16),
            jax.ShapeDtypeStruct((n_rep, blocks, height, width), bf16),
        ),
        in_specs=[pl.BlockSpec(memory_space=pltpu.SMEM)] + [any_spec] * 5,
        out_specs=(vmem_spec, vmem_spec),
        scratch_shapes=[
            pltpu.VMEM((outer, GROUP * tok, cols), bf16),
            pltpu.VMEM((GROUP * tok, key_width), bf16),
            pltpu.VMEM((slots, n, height, width), bf16),
            pltpu.VMEM(slot_grads.shape, bf16),
            pltpu.VMEM(right_root.shape, bf16),
            pltpu.VMEM((n, slots, height, width), bf16),
            pltpu.VMEM((n * slots, height, width), bf16),
            pltpu.VMEM((blocks, height, width), bf16),
            pltpu.VMEM((blocks, height, width), bf16),
            pltpu.VMEM((outer, PIECES, cols, piece), bf16),
            pltpu.VMEM((outer, PIECES, cols, piece), bf16),
            pltpu.VMEM((outer, PIECES, cols, piece), f32),
            pltpu.VMEM((outer - 1, PIECES, cols, piece), bf16),
            pltpu.VMEM((outer, PIECES, cols, piece), bf16),
            pltpu.VMEM((PIECES, cols, piece), bf16),
            pltpu.VMEM((PIECES, cols, piece), bf16),
            dma((4,)),
            dma((outer,)),
            dma,
            dma((3,)),
            dma((GROUP,)),
            dma((outer, 3)),
            dma((GROUP, outer)),
            dma((n,)),
            dma((n,)),
            dma((outer, PIECES)),
            dma((outer, PIECES)),
            dma((outer - 1, PIECES)),
            dma((outer, PIECES)),
            dma((PIECES,)),
            dma((PIECES,)),
            dma,
            dma,
        ],
        compiler_params=pltpu.CompilerParams(
            collective_id=0, has_side_effects=True, vmem_limit_bytes=60 * 1024 * 1024
        ),
    )(
        block_slot,
        tokens_x,
        key_grad,
        left_root.reshape(slots, n, n_rep, height, width),
        slot_grads,
        right_root,
    )
    grad_key = sums.astype(f32)
    update = jnp.transpose(rows, (0, 2, 1, 3)).reshape(n_rep * height, blocks, width)
    return (grad_key, update)


def shards(tokens_x, key_grad, left_root, slot_grads, right_root, block_slot):
    n = lax.axis_size("shard")
    n_rep = lax.axis_size("rep")
    aligned = (
        n_rep == 2
        and n % GROUP == 0
        and n > GROUP
        and tokens_x.shape[1] % (n * 128) == 0
        and key_grad.shape[1] % (n_rep * PIECES * 128) == 0
        and tokens_x.shape[0] % 16 == 0
        and left_root.shape[1] % (n * n_rep * 16) == 0
        and left_root.shape[2] % 128 == 0
    )
    program = fused_shards if aligned else plain_shards
    return program(tokens_x, key_grad, left_root, slot_grads, right_root, block_slot)


def solution(mesh):
    return jax.shard_map(
        shards,
        mesh=mesh,
        in_specs=(
            P(("rep", "shard"), None),
            P(("rep", "shard"), None),
            P("shard", None, None),
            P("shard", None, None),
            P("shard", None, None),
            P(),
        ),
        out_specs=(P("shard", None), P("shard", None, None)),
        check_vma=False,
    )
```

```python
import functools

import jax
import jax.numpy as jnp
from jax import lax
from jax.experimental import pallas as pl
from jax.experimental.pallas import tpu as pltpu
from jax.sharding import PartitionSpec as P

MESH = pl.DeviceIdType.MESH
GROUP = 4
PIECES = 2


def column_term(features, cotangent):
    return lax.dot_general(
        features, cotangent, (((0,), (0,)), ((), ())), preferred_element_type=jnp.float32
    )


def precondition(left_block, grad_block, right_block):
    left_part = jnp.einsum(
        "sij,sjk->sik", left_block, grad_block, preferred_element_type=jnp.float32
    ).astype(jnp.bfloat16)
    return jnp.einsum(
        "sij,sjk->isk", left_part, right_block, preferred_element_type=jnp.float32
    ).astype(jnp.bfloat16)


def plain_shards(tokens_x, key_grad, left_root, slot_grads, right_root, block_slot):
    n_shard = lax.axis_size("shard")
    n_rep = lax.axis_size("rep")
    own_rows = lax.psum_scatter(
        column_term(tokens_x, key_grad), "shard", scatter_dimension=0, tiled=True
    )
    grad_key = lax.psum(own_rows, "rep")
    slot_count = left_root.shape[0]
    half_slots = slot_count // n_rep
    first_slot = lax.axis_index("rep") * half_slots

    def own_half(values):
        return lax.dynamic_slice_in_dim(values, first_slot, half_slots, 0)

    product = precondition(own_half(left_root), own_half(slot_grads), own_half(right_root))
    received = lax.all_to_all(product, "shard", split_axis=0, concat_axis=1, tiled=True)
    joined = lax.all_gather(received, "rep", axis=1, tiled=True)
    owner = block_slot // slot_count
    within = block_slot % slot_count
    position = (
        within // half_slots * (n_shard * half_slots) + owner * half_slots + within % half_slots
    )
    update = jnp.take(joined, position, axis=1)
    return (grad_key, update)


def remote(src, dst, send_sem, recv_sem, axis, index):
    return pltpu.make_async_remote_copy(
        src_ref=src,
        dst_ref=dst,
        send_sem=send_sem,
        recv_sem=recv_sem,
        device_id={axis: index},
        device_id_type=MESH,
    )


def far_first(outer):
    return sorted(range(1, outer), key=lambda off: -min(off, outer - off)) + [0]


def kernel(
    n, slot_ref, x_ref, g_ref, lr_ref, sg_ref, rr_ref, og_ref, ou_ref,
    x_all, g_all, lr, sg, rr, prod, upd, mine, theirs, part, met, kept, passed, landed, half_out, half_in,
    local_sem, x_local, barrier_free, g_send, g_recv, x_send, x_recv, u_send, u_recv,
    a_send, a_recv, z_send, z_recv, r_send, r_recv, v_send, v_recv,
):
    me = lax.axis_index("shard")
    rep = lax.axis_index("rep")
    other_rep = 1 - rep
    q = me % GROUP
    z = me // GROUP
    base = z * GROUP
    outer = n // GROUP
    q_core = q + 1 - 2 * (q % 2)
    q_far = (q + 2) % GROUP
    q_both = (q_core + 2) % GROUP
    tok = x_ref.shape[0]
    cols = x_ref.shape[1] // n
    slots = lr_ref.shape[0]
    blocks = slot_ref.shape[0]
    offsets = far_first(outer)

    def tokens_of(index):
        return pl.ds(index * tok, tok)

    def columns(d, index):
        return pl.ds(pl.multiple_of((d * GROUP + index) * cols, 128), cols)

    copy_lr = pltpu.make_async_copy(lr_ref.at[:, :, rep], lr, local_sem.at[0])
    copy_sg = pltpu.make_async_copy(sg_ref, sg, local_sem.at[1])
    copy_rr = pltpu.make_async_copy(rr_ref, rr, local_sem.at[2])
    copy_g = pltpu.make_async_copy(g_ref, g_all.at[tokens_of(q)], local_sem.at[3])
    copies_x = []
    for d in range(outer):
        copies_x.append(
            pltpu.make_async_copy(
                x_ref.at[:, columns(d, q)], x_all.at[d, tokens_of(q)], x_local.at[d]
            )
        )
    copy_lr.start()
    copy_sg.start()
    copy_rr.start()
    copy_g.start()
    for copy in copies_x:
        copy.start()

    barrier = pltpu.get_barrier_semaphore()
    for step in range(1, n):
        pl.semaphore_signal(
            barrier, inc=1, device_id={"shard": (me + step) % n}, device_id_type=MESH
        )
    pl.semaphore_signal(barrier, inc=1, device_id={"rep": other_rep}, device_id_type=MESH)
    pl.semaphore_wait(barrier, n)

    sent = []

    def send(*args):
        copy = remote(*args)
        copy.start()
        sent.append(copy)

    for order, target in enumerate((q_far, q_core)):
        send(
            g_ref, g_all.at[tokens_of(q)], g_send.at[order], g_recv.at[q], "shard", base + target
        )
    for order, off in enumerate(offsets):
        d = (z + off) % outer
        for place, target in enumerate((q_far, q_both, q_core)):
            send(
                x_ref.at[:, columns(d, target)],
                x_all.at[d, tokens_of(q)],
                x_send.at[order, place],
                x_recv.at[q, d],
                "shard",
                base + target,
            )

    copy_lr.wait()
    copy_sg.wait()
    copy_rr.wait()
    height = lr.shape[2]
    width = lr.shape[3]
    for s in range(slots):
        left = jnp.dot(
            lr[s].reshape(n * height, width), sg[s], preferred_element_type=jnp.float32
        ).astype(jnp.bfloat16)
        both = jnp.dot(left, rr[s], preferred_element_type=jnp.float32).astype(jnp.bfloat16)
        prod[:, s] = both.reshape(n, height, width)
    for step in range(1, n):
        target = (me + step) % n
        send(
            prod.at[target],
            upd.at[pl.ds(me * slots, slots)],
            u_send.at[step],
            u_recv.at[me],
            "shard",
            target,
        )
    upd[pl.ds(me * slots, slots)] = prod[me]

    def arrive(dst, recv_sem):
        remote(dst, dst, barrier_free, recv_sem, "shard", (me + 1) % n).wait_recv()

    arrive(g_all.at[tokens_of(q_far)], g_recv.at[q_far])
    send(
        g_all.at[tokens_of(q_far)],
        g_all.at[tokens_of(q_far)],
        g_send.at[2],
        g_recv.at[q_far],
        "shard",
        base + q_core,
    )
    copy_g.wait()
    arrive(g_all.at[tokens_of(q_core)], g_recv.at[q_core])
    arrive(g_all.at[tokens_of(q_both)], g_recv.at[q_both])
    for copy in copies_x:
        copy.wait()

    piece = kept.shape[3]
    half = PIECES * piece

    def partial(d, side):
        start = pl.multiple_of(side * half, 128)
        return lax.dot_general(
            x_all[d],
            g_all[:, pl.ds(start, half)],
            (((0,), (0,)), ((), ())),
            preferred_element_type=jnp.float32,
        )

    def place_of(side, p):
        return pl.ds(pl.multiple_of(side * half + p * piece, 128), piece)

    def pass_on(order):
        off = offsets[order]
        for p in range(PIECES):
            arrive(met.at[order, p], a_recv.at[order, p])
            total = kept[order, p] + met[order, p].astype(jnp.float32)
            if off == 0:
                kept[order, p] = total
            else:
                passed[order, p] = total.astype(jnp.bfloat16)
                send(
                    passed.at[order, p],
                    landed.at[z, p],
                    z_send.at[order, p],
                    z_recv.at[z, p],
                    "shard",
                    (z + off) % outer * GROUP + q,
                )

    for order, off in enumerate(offsets):
        d = (z + off) % outer
        for source in (q_core, q_far, q_both):
            arrive(x_all.at[d, tokens_of(source)], x_recv.at[source, d])
        value = partial(d, other_rep)
        for p in range(PIECES):
            part[order, p] = value[:, p * piece : (p + 1) * piece].astype(jnp.bfloat16)
            send(
                part.at[order, p],
                met.at[order, p],
                a_send.at[order, p],
                a_recv.at[order, p],
                "rep",
                other_rep,
            )
        value = partial(d, rep)
        for p in range(PIECES):
            kept[order, p] = value[:, p * piece : (p + 1) * piece]
        if order > 0:
            pass_on(order - 1)
    pass_on(outer - 1)

    for p in range(PIECES):
        total = kept[outer - 1, p]
        for off in offsets[:-1]:
            source = (z + outer - off) % outer
            arrive(landed.at[source, p], z_recv.at[source, p])
            total = total + landed[source, p].astype(jnp.float32)
        half_out[p] = total.astype(jnp.bfloat16)
        send(half_out.at[p], half_in.at[p], r_send.at[p], r_recv.at[p], "rep", other_rep)

    for step in range(1, n):
        source = (me + n - step) % n
        arrive(upd.at[pl.ds(source * slots, slots)], u_recv.at[source])

    def pick(b, carry):
        mine[b] = upd[slot_ref[b]]
        return carry

    lax.fori_loop(0, blocks, pick, 0)
    send(mine, theirs, v_send, v_recv, "rep", other_rep)
    ou_ref[rep] = mine[...]

    for p in range(PIECES):
        og_ref[:, place_of(rep, p)] = half_out[p]
    arrive(theirs, v_recv)
    ou_ref[other_rep] = theirs[...]
    for p in range(PIECES):
        arrive(half_in.at[p], r_recv.at[p])
        og_ref[:, place_of(other_rep, p)] = half_in[p]
    for copy in sent:
        copy.wait_send()


def fused_shards(tokens_x, key_grad, left_root, slot_grads, right_root, block_slot):
    n = lax.axis_size("shard")
    n_rep = lax.axis_size("rep")
    outer = n // GROUP
    tok, d_model = tokens_x.shape
    key_width = key_grad.shape[1]
    cols = d_model // n
    slots, order_b, width = left_root.shape
    height = order_b // n // n_rep
    blocks = block_slot.shape[0]
    piece = key_width // n_rep // PIECES
    bf16, f32 = jnp.bfloat16, jnp.float32
    dma = pltpu.SemaphoreType.DMA
    any_spec = pl.BlockSpec(memory_space=pl.ANY)
    vmem_spec = pl.BlockSpec(memory_space=pltpu.VMEM)
    sums, rows = pl.pallas_call(
        functools.partial(kernel, n),
        out_shape=(
            jax.ShapeDtypeStruct((cols, key_width), bf16),
            jax.ShapeDtypeStruct((n_rep, blocks, height, width), bf16),
        ),
        in_specs=[pl.BlockSpec(memory_space=pltpu.SMEM)] + [any_spec] * 5,
        out_specs=(vmem_spec, vmem_spec),
        scratch_shapes=[
            pltpu.VMEM((outer, GROUP * tok, cols), bf16),
            pltpu.VMEM((GROUP * tok, key_width), bf16),
            pltpu.VMEM((slots, n, height, width), bf16),
            pltpu.VMEM(slot_grads.shape, bf16),
            pltpu.VMEM(right_root.shape, bf16),
            pltpu.VMEM((n, slots, height, width), bf16),
            pltpu.VMEM((n * slots, height, width), bf16),
            pltpu.VMEM((blocks, height, width), bf16),
            pltpu.VMEM((blocks, height, width), bf16),
            pltpu.VMEM((outer, PIECES, cols, piece), bf16),
            pltpu.VMEM((outer, PIECES, cols, piece), bf16),
            pltpu.VMEM((outer, PIECES, cols, piece), f32),
            pltpu.VMEM((outer - 1, PIECES, cols, piece), bf16),
            pltpu.VMEM((outer, PIECES, cols, piece), bf16),
            pltpu.VMEM((PIECES, cols, piece), bf16),
            pltpu.VMEM((PIECES, cols, piece), bf16),
            dma((4,)),
            dma((outer,)),
            dma,
            dma((3,)),
            dma((GROUP,)),
            dma((outer, 3)),
            dma((GROUP, outer)),
            dma((n,)),
            dma((n,)),
            dma((outer, PIECES)),
            dma((outer, PIECES)),
            dma((outer - 1, PIECES)),
            dma((outer, PIECES)),
            dma((PIECES,)),
            dma((PIECES,)),
            dma,
            dma,
        ],
        compiler_params=pltpu.CompilerParams(
            collective_id=0, has_side_effects=True, vmem_limit_bytes=60 * 1024 * 1024
        ),
    )(
        block_slot,
        tokens_x,
        key_grad,
        left_root.reshape(slots, n, n_rep, height, width),
        slot_grads,
        right_root,
    )
    grad_key = sums.astype(f32)
    update = jnp.transpose(rows, (0, 2, 1, 3)).reshape(n_rep * height, blocks, width)
    return (grad_key, update)


def shards(tokens_x, key_grad, left_root, slot_grads, right_root, block_slot):
    n = lax.axis_size("shard")
    n_rep = lax.axis_size("rep")
    aligned = (
        n_rep == 2
        and n % GROUP == 0
        and n > GROUP
        and tokens_x.shape[1] % (n * 128) == 0
        and key_grad.shape[1] % (n_rep * PIECES * 128) == 0
        and tokens_x.shape[0] % 16 == 0
        and left_root.shape[1] % (n * n_rep * 16) == 0
        and left_root.shape[2] % 128 == 0
    )
    program = fused_shards if aligned else plain_shards
    return program(tokens_x, key_grad, left_root, slot_grads, right_root, block_slot)


def solution(mesh):
    return jax.shard_map(
        shards,
        mesh=mesh,
        in_specs=(
            P(("rep", "shard"), None),
            P(("rep", "shard"), None),
            P("shard", None, None),
            P("shard", None, None),
            P("shard", None, None),
            P(),
        ),
        out_specs=(P("shard", None), P("shard", None, None)),
        check_vma=False,
    )
```
